32 devices in a mesh: node: 4 (over y, x), space: 8 (over z, core).
Axes of the slice: x: 2, y: 2, z: 4, core: 2. Of those that a mesh axis runs over, the one named last changes fastest.
Arguments:
- initial: float32 [2, 512, 4096], P(None, 'space'), may hold values from 0 to 1
- sections: float32 [4, 2, 512, 4096], P('node', None, 'space'), may hold values from 0 to 1
- feed_rate: float32 [512, 4096], P('space'), may hold values from 0.02 to 0.12
- kill_rate: float32 [512, 4096], P('space'), may hold values from 0.04 to 0.12
Outputs:
- new_sections: float32 [4, 2, 512, 4096], P('node', None, 'space')
- residual_max: float32 [], replicated
The draws below stay inside these ranges and needn't reach their ends.
All inputs are finite; a program needn't handle non-finite values.
Results may differ from the reference program's by a relative error of at most 0.000094.
Values sent between devices are 32-bit elements; how exact they have to be, the bound alone decides.
A program may use at most 64 MiB of HBM per device.

```python
import math
import jax
import jax.numpy as jnp
import numpy as np
from jax import lax

NY = 4096
SWEEPS = 6
M = 4
NX = 512


def steps_of(key, extent, cuts, low, high):
    def one(position, shards_of):
        draws = jax.random.uniform(jax.random.fold_in(jax.random.fold_in(key, 6), position), (shards_of,), jnp.float32, low / len(cuts), high / len(cuts))
        return jnp.repeat(jnp.exp(draws), extent[position] // shards_of).reshape((-1,) + (1,) * (len(extent) - position - 1))

    level = one(*cuts[0])
    for cut in cuts[1:]:
        level = level * one(*cut)
    return level


def setup_inputs(seed: int = 0) -> dict:
    arg_keys = jax.random.split(jax.random.key(seed), 5)
    return {
        "initial": jnp.clip(1.0 * jax.random.uniform(arg_keys[0], (2, NX, NY), jnp.float32) ** steps_of(arg_keys[0], (2, NX, NY), ((1, 8),), -0.2, 0.2), 0.0, 1.0),
        "sections": jnp.clip(1.0 * jax.random.uniform(arg_keys[1], (M, 2, NX, NY), jnp.float32) ** steps_of(arg_keys[1], (M, 2, NX, NY), ((0, 4), (2, 8)), -0.2, 0.2), 0.0, 1.0),
        "feed_rate": jnp.clip(jnp.exp(math.log(0.12) - 1.7917595 * jax.random.uniform(arg_keys[2], (NX, NY), jnp.float32) ** steps_of(arg_keys[2], (NX, NY), ((0, 8),), -0.2, 0.2)), 0.02, 0.12),
        "kill_rate": jnp.clip(jnp.exp(math.log(0.12) - 1.0986123 * jax.random.uniform(arg_keys[3], (NX, NY), jnp.float32) ** steps_of(arg_keys[3], (NX, NY), ((0, 8),), -0.2, 0.2)), 0.04, 0.12),
    }


step_size = 4.0
diff_u = 1.0
diff_v = 0.5


def radau_target(order, value):
    before = 1.0
    current = value
    previous = 1.0
    for degree in range(1, order):
        following = ((2 * degree + 1) * value * current - degree * before) / (degree + 1)
        before = current
        current = following
    if order == 1:
        previous = 1.0
    else:
        previous = before
    return current - previous


def radau_table(total):
    grid_count = 20000
    roots_found = []
    left_value = -1.0
    left_target = radau_target(total, left_value)
    for step_index in range(1, grid_count):
        right_value = -1.0 + 2.0 * step_index / grid_count
        right_target = radau_target(total, right_value)
        if left_target * right_target < 0.0:
            lower = left_value
            upper = right_value
            lower_target = left_target
            for bisect_index in range(80):
                halfway = 0.5 * (lower + upper)
                halfway_target = radau_target(total, halfway)
                if lower_target * halfway_target <= 0.0:
                    upper = halfway
                else:
                    lower = halfway
                    lower_target = halfway_target
            roots_found.append(0.5 * (lower + upper))
        left_value = right_value
        left_target = right_target
    roots_found.append(1.0)
    points = [(value + 1.0) / 2.0 for value in roots_found]
    quad_rows = []
    for node_index in range(total):
        row_values = []
        for basis_index in range(total):
            coefs = [1.0]
            for other_index in range(total):
                if other_index != basis_index:
                    scale = 1.0 / (points[basis_index] - points[other_index])
                    shifted = [0.0] + coefs
                    widened = coefs + [0.0]
                    coefs = [(shifted[k] - points[other_index] * widened[k]) * scale for k in range(len(shifted))]
            integral = 0.0
            for power_index in range(len(coefs)):
                integral += coefs[power_index] * points[node_index] ** (power_index + 1) / (power_index + 1)
            row_values.append(integral)
        quad_rows.append(row_values)
    return np.array(points), np.array(quad_rows)


def neighbours(field):
    return (jnp.roll(field, -1, 2) + jnp.roll(field, 1, 2)) + (jnp.roll(field, -1, 3) + jnp.roll(field, 1, 3))


def reference(initial, sections, feed_rate, kill_rate):
    points, quad_matrix = radau_table(M)
    points = jnp.asarray(points, jnp.float32)
    quad_matrix = jnp.asarray(quad_matrix, jnp.float32)
    diffusivity = jnp.array([diff_u, diff_v], jnp.float32).reshape(1, 2, 1, 1)
    laplace = neighbours(sections) - 4.0 * sections
    implicit = diffusivity * laplace
    species_u = sections[:, 0]
    species_v = sections[:, 1]
    product = species_u * species_v * species_v
    reaction = jnp.stack((-product + feed_rate * (1.0 - species_u), product - (feed_rate + kill_rate) * species_v), axis=1)
    slopes = implicit + reaction
    summed = jnp.einsum("mj,jsxy->msxy", quad_matrix, slopes, precision=lax.Precision.HIGHEST)
    quadrature = initial[None] + step_size * summed
    residual_max = jnp.max(jnp.abs(quadrature - sections))
    node_step = (step_size * points).reshape(M, 1, 1, 1)
    right_side = quadrature - node_step * implicit
    coupling = node_step * diffusivity
    divisor = 4.0 * coupling + 1.0
    iterate = sections
    for sweep_index in range(SWEEPS):
        iterate = (right_side + coupling * neighbours(iterate)) / divisor
    return iterate, residual_max
```

```python
import functools

import jax
import jax.numpy as jnp
import numpy as np
from jax import lax
from jax.experimental import pallas as pl
from jax.experimental.pallas import tpu as pltpu
from jax.sharding import PartitionSpec as P

SWEEPS = 6


step_size = 4.0
diff_u = 1.0
diff_v = 0.5


def radau_target(order, value):
    before = 1.0
    current = value
    previous = 1.0
    for degree in range(1, order):
        following = ((2 * degree + 1) * value * current - degree * before) / (degree + 1)
        before = current
        current = following
    previous = before
    return current - previous


def radau_table(total):
    grid_count = 20000
    roots_found = []
    left_value = -1.0
    left_target = radau_target(total, left_value)
    for step_index in range(1, grid_count):
        right_value = -1.0 + 2.0 * step_index / grid_count
        right_target = radau_target(total, right_value)
        if left_target * right_target < 0.0:
            lower = left_value
            upper = right_value
            lower_target = left_target
            for bisect_index in range(80):
                halfway = 0.5 * (lower + upper)
                halfway_target = radau_target(total, halfway)
                if lower_target * halfway_target <= 0.0:
                    upper = halfway
                else:
                    lower = halfway
                    lower_target = halfway_target
            roots_found.append(0.5 * (lower + upper))
        left_value = right_value
        left_target = right_target
    roots_found.append(1.0)
    points = [(value + 1.0) / 2.0 for value in roots_found]
    quad_rows = []
    for node_index in range(total):
        row_values = []
        for basis_index in range(total):
            coefs = [1.0]
            for other_index in range(total):
                if other_index != basis_index:
                    scale = 1.0 / (points[basis_index] - points[other_index])
                    shifted = [0.0] + coefs
                    widened = coefs + [0.0]
                    coefs = [
                        (shifted[k] - points[other_index] * widened[k]) * scale
                        for k in range(len(shifted))
                    ]
            integral = 0.0
            for power_index in range(len(coefs)):
                integral += (
                    coefs[power_index] * points[node_index] ** (power_index + 1) / (power_index + 1)
                )
            row_values.append(integral)
        quad_rows.append(row_values)
    return (np.array(points), np.array(quad_rows))


MESH = pl.DeviceIdType.MESH
LANES = 128
EDGE = 8
TOP = 2 * EDGE


def kernel(
    nodes,
    spaces,
    table,
    sections,
    feed_rate,
    kill_rate,
    initial,
    out,
    residual,
    sec,
    feed,
    kill,
    init,
    side,
    slope,
    arrived,
    mixed,
    quad,
    work,
    final,
    peak,
    peaks_node,
    peaks_space,
    local_sem,
    out_sem,
    halo_sem,
    first_sem,
    second_sem,
    side_sem,
    peak_node_sem,
    peak_space_sem,
):
    cols = sec.shape[1]
    rows = slope.shape[2]
    block = cols // nodes
    me = lax.axis_index("node")
    here = lax.axis_index("space")
    tall = 2 if nodes % 2 == 0 else 1
    wide = nodes // tall
    pieces = ((EDGE, rows - 2 * EDGE), (0, EDGE), (rows - EDGE, EDGE))
    mid, edges = 0, (1, 2)

    def ahead(o):
        return ((me // wide + o // wide) % tall) * wide + (me % wide + o % wide) % wide

    def behind(o):
        return ((me // wide + tall - o // wide) % tall) * wide + (
            me % wide + wide - o % wide
        ) % wide

    def fetch(source, target, sem):
        def one(c, carry):
            at = pl.ds(pl.multiple_of(c * LANES, LANES), LANES)
            pltpu.make_async_copy(source.at[:, at], target(c), sem).start()
            return carry

        lax.fori_loop(0, cols, one, 0)

    own_rows = pl.ds(TOP, rows)
    for s in range(2):
        fetch(sections.at[0, s], lambda c: sec.at[s, c, own_rows], local_sem.at[s])
    fetch(feed_rate, lambda c: feed.at[c], local_sem.at[2])
    fetch(kill_rate, lambda c: kill.at[c], local_sem.at[3])

    barrier = pltpu.get_barrier_semaphore()
    for o in range(1, nodes):
        pl.semaphore_signal(barrier, inc=1, device_id={"node": ahead(o)}, device_id_type=MESH)
    for o in range(1, spaces):
        pl.semaphore_signal(
            barrier, inc=1, device_id={"space": (here + o) % spaces}, device_id_type=MESH
        )

    def arrived_in(ref, sem):
        pltpu.make_async_copy(ref, ref, sem).wait()

    def halo(ref, sem, s, way):
        start = TOP + rows - EDGE if way == 0 else TOP
        land = TOP - EDGE if way == 0 else TOP + rows
        other = (here + 1) % spaces if way == 0 else (here + spaces - 1) % spaces
        return pltpu.make_async_remote_copy(
            src_ref=ref.at[s, :, pl.ds(start, EDGE)],
            dst_ref=ref.at[s, :, pl.ds(land, EDGE)],
            send_sem=sem.at[0, s, way],
            recv_sem=sem.at[1, s, way],
            device_id={"space": other},
            device_id_type=MESH,
        )

    def first(s, p, o):
        start, size = pieces[p]
        return pltpu.make_async_remote_copy(
            src_ref=slope.at[s, pl.ds(ahead(o) * block, block), pl.ds(start, size)],
            dst_ref=arrived.at[o - 1, s, :, pl.ds(start, size)],
            send_sem=first_sem.at[0, s, p, o - 1],
            recv_sem=first_sem.at[1, s, p, o - 1],
            device_id={"node": ahead(o)},
            device_id_type=MESH,
        )

    def second(s, p, o):
        start, size = pieces[p]
        return pltpu.make_async_remote_copy(
            src_ref=mixed.at[o - 1, s, :, pl.ds(start, size)],
            dst_ref=quad.at[s, pl.ds(me * block, block), pl.ds(start, size)],
            send_sem=second_sem.at[0, s, p, o - 1],
            recv_sem=second_sem.at[1, s, p, o - 1],
            device_id={"node": ahead(o)},
            device_id_type=MESH,
        )

    arrived_in(sec.at[0, :, own_rows], local_sem.at[0])
    arrived_in(sec.at[1, :, own_rows], local_sem.at[1])
    pl.semaphore_wait(barrier, nodes - 1 + spaces - 1)
    for s in range(2):
        for way in range(2):
            halo(sec, halo_sem, s, way).start()
    arrived_in(feed, local_sem.at[2])
    arrived_in(kill, local_sem.at[3])
    for s in range(2):
        fetch(initial.at[s], lambda c: init.at[s, c], local_sem.at[4 + s])

    own_step = table[nodes * nodes + me]
    coupling = (own_step * diff_u, own_step * diff_v)

    def around(ref, c, start, size):
        lane = lax.broadcasted_iota(jnp.int32, (size, LANES), 1)
        centre = ref(c, start, size)
        left = ref((c + cols - 1) % cols, start, size)
        right = ref((c + 1) % cols, start, size)
        left = pltpu.roll(jnp.where(lane == LANES - 1, left, centre), 1, 1)
        right = pltpu.roll(jnp.where(lane == 0, right, centre), LANES - 1, 1)
        vertical = ref(c, start + 1, size) + ref(c, start - 1, size)
        return centre, vertical + (right + left)

    def slopes(owner, p):
        start, size = pieces[p]

        def one(k, carry):
            c = owner * block + k
            u, u_ring = around(lambda *a: sec[0, a[0], pl.ds(a[1], a[2]), :], c, TOP + start, size)
            v, v_ring = around(lambda *a: sec[1, a[0], pl.ds(a[1], a[2]), :], c, TOP + start, size)
            f = feed[c, pl.ds(start, size), :]
            k_ = kill[c, pl.ds(start, size), :]
            u_lap = diff_u * (u_ring - 4.0 * u)
            v_lap = diff_v * (v_ring - 4.0 * v)
            product = u * v * v
            slope[0, c, pl.ds(start, size), :] = u_lap + (f * (1.0 - u) - product)
            slope[1, c, pl.ds(start, size), :] = v_lap + (product - (f + k_) * v)
            side[0, c, pl.ds(TOP + start, size), :] = own_step * u_lap
            side[1, c, pl.ds(TOP + start, size), :] = own_step * v_lap
            return carry

        lax.fori_loop(0, block, one, 0)

    order = tuple(range(nodes - 1, 0, -1))
    for o in order:
        slopes(ahead(o), mid)
        first(0, mid, o).start()
    for s in range(2):
        for way in range(2):
            halo(sec, halo_sem, s, way).wait_recv()
    for o in order:
        for p in edges:
            slopes(ahead(o), p)
            first(0, p, o).start()
    for o in order:
        first(1, mid, o).start()
    for o in order:
        for p in edges:
            first(1, p, o).start()
    for p in range(3):
        slopes(me, p)

    def mix(s, p):
        start, size = pieces[p]
        at = pl.ds(start, size)
        sources = [me] + [behind(o) for o in range(1, nodes)]
        targets = [me] + [ahead(o) for o in range(1, nodes)]

        def one(k, carry):
            values = [slope[s, me * block + k, at, :]] + [
                arrived[o - 1, s, k, at, :] for o in range(1, nodes)
            ]
            for t, m in enumerate(targets):
                total = table[m * nodes + sources[0]] * values[0]
                for j in range(1, nodes):
                    total = total + table[m * nodes + sources[j]] * values[j]
                if t == 0:
                    quad[s, me * block + k, at, :] = total
                else:
                    mixed[t - 1, s, k, at, :] = total
            return carry

        lax.fori_loop(0, block, one, 0)

    for s in range(2):
        for o in order:
            for p in edges + (mid,):
                first(s, p, o).wait_recv()
        for p in edges + (mid,):
            mix(s, p)
            for o in order:
                second(s, p, o).start()

    inverse = [1.0 / (4.0 * c + 1.0) for c in coupling]

    def gather(s, p, worst):
        start, size = pieces[p]
        at = pl.ds(start, size)
        for o in order:
            second(s, p, o).wait_recv()

        def one(c, worst):
            whole = init[s, c, at, :] + quad[s, c, at, :]
            gap = jnp.abs(whole - sec[s, c, pl.ds(TOP + start, size), :])
            where = pl.ds(TOP + start, size)
            side[s, c, where, :] = (whole - side[s, c, where, :]) * inverse[s]
            return jnp.maximum(worst, jnp.max(gap.reshape(size // EDGE, EDGE, LANES), axis=0))

        return lax.fori_loop(0, cols, one, worst)

    def sweep(s, source, target, first_row, size):
        factor = coupling[s] * inverse[s]

        def one(c, carry):
            _, ring = around(source, c, first_row, size)
            target(c, side[s, c, pl.ds(first_row, size), :] + factor * ring)
            return carry

        lax.fori_loop(0, cols, one, 0)

    def peak_node(o):
        return pltpu.make_async_remote_copy(
            src_ref=peak.at[0],
            dst_ref=peaks_node.at[o - 1],
            send_sem=peak_node_sem.at[0, o - 1],
            recv_sem=peak_node_sem.at[1, o - 1],
            device_id={"node": ahead(o)},
            device_id_type=MESH,
        )

    def peak_space(o):
        return pltpu.make_async_remote_copy(
            src_ref=peak.at[1],
            dst_ref=peaks_space.at[o - 1],
            send_sem=peak_space_sem.at[0, o - 1],
            recv_sem=peak_space_sem.at[1, o - 1],
            device_id={"space": (here + o) % spaces},
            device_id_type=MESH,
        )

    def fold_node():
        for o in range(1, nodes):
            peak_node(o).wait_recv()
        peak[1] = jnp.maximum(peak[0], jnp.max(peaks_node[...], axis=0))
        for o in range(1, spaces):
            peak_space(o).start()

    worst = jnp.zeros((EDGE, LANES), jnp.float32)
    last_row = TOP - EDGE
    for s in range(2):
        arrived_in(init.at[s], local_sem.at[4 + s])
        for p in edges:
            worst = gather(s, p, worst)
        for way in range(2):
            halo(side, side_sem, s, way).start()
        worst = gather(s, mid, worst)
        if s == 1:
            peak[0] = worst
            for o in range(1, nodes):
                peak_node(o).start()
        for way in range(2):
            halo(side, side_sem, s, way).wait_recv()

        def from_work(b):
            return lambda c, start, size: work[b, c, pl.ds(start, size), :]

        def into_work(b):
            def put(c, value):
                work[b, c, pl.ds(TOP - EDGE, rows + 2 * EDGE), :] = value

            return put

        def put_final(c, value):
            final[s, c] = value
            at = pl.ds(pl.multiple_of(c * LANES, LANES), LANES)
            pltpu.make_async_copy(final.at[s, c], out.at[0, s, :, at], out_sem.at[s]).start()

        for index in range(SWEEPS):
            if index == 0:
                source = lambda c, start, size: sec[s, c, pl.ds(start, size), :]
            else:
                source = from_work((index + 1) % 2)
            if index == SWEEPS - 1:
                if s == 1:
                    fold_node()
                sweep(s, source, put_final, TOP, rows)
            else:
                sweep(s, source, into_work(index % 2), TOP - EDGE, rows + 2 * EDGE)

    for o in range(1, spaces):
        peak_space(o).wait_recv()
    residual[...] = jnp.maximum(peak[1], jnp.max(peaks_space[...], axis=0))
    for s in range(2):
        for way in range(2):
            halo(sec, halo_sem, s, way).wait_send()
            halo(side, side_sem, s, way).wait_send()
        for p in range(3):
            for o in order:
                first(s, p, o).wait_send()
                second(s, p, o).wait_send()
    for o in range(1, nodes):
        peak_node(o).wait_send()
    for o in range(1, spaces):
        peak_space(o).wait_send()
    for s in range(2):
        arrived_in(final.at[s], out_sem.at[s])


def shards(initial, sections, feed_rate, kill_rate):
    nodes = lax.axis_size("node")
    spaces = lax.axis_size("space")
    rows, columns = feed_rate.shape
    cols = columns // LANES
    block = cols // nodes
    points, quad_matrix = radau_table(nodes)
    table = np.concatenate(
        [
            step_size * np.float32(quad_matrix).reshape(-1),
            step_size * np.float32(points),
        ]
    ).astype(np.float32)
    high = TOP + rows + TOP
    f32 = jnp.float32
    any_spec = pl.BlockSpec(memory_space=pl.ANY)
    result, residual = pl.pallas_call(
        functools.partial(kernel, nodes, spaces),
        out_shape=(
            jax.ShapeDtypeStruct(sections.shape, f32),
            jax.ShapeDtypeStruct((EDGE, LANES), f32),
        ),
        in_specs=[pl.BlockSpec(memory_space=pltpu.SMEM)] + [any_spec] * 4,
        out_specs=(any_spec, pl.BlockSpec(memory_space=pltpu.VMEM)),
        scratch_shapes=[
            pltpu.VMEM((2, cols, high, LANES), f32),
            pltpu.VMEM((cols, rows, LANES), f32),
            pltpu.VMEM((cols, rows, LANES), f32),
            pltpu.VMEM((2, cols, rows, LANES), f32),
            pltpu.VMEM((2, cols, high, LANES), f32),
            pltpu.VMEM((2, cols, rows, LANES), f32),
            pltpu.VMEM((nodes - 1, 2, block, rows, LANES), f32),
            pltpu.VMEM((nodes - 1, 2, block, rows, LANES), f32),
            pltpu.VMEM((2, cols, rows, LANES), f32),
            pltpu.VMEM((2, cols, high, LANES), f32),
            pltpu.VMEM((2, cols, rows, LANES), f32),
            pltpu.VMEM((2, EDGE, LANES), f32),
            pltpu.VMEM((nodes - 1, EDGE, LANES), f32),
            pltpu.VMEM((spaces - 1, EDGE, LANES), f32),
            pltpu.SemaphoreType.DMA((6,)),
            pltpu.SemaphoreType.DMA((2,)),
            pltpu.SemaphoreType.DMA((2, 2, 2)),
            pltpu.SemaphoreType.DMA((2, 2, 3, nodes - 1)),
            pltpu.SemaphoreType.DMA((2, 2, 3, nodes - 1)),
            pltpu.SemaphoreType.DMA((2, 2, 2)),
            pltpu.SemaphoreType.DMA((2, nodes - 1)),
            pltpu.SemaphoreType.DMA((2, spaces - 1)),
        ],
        compiler_params=pltpu.CompilerParams(
            collective_id=0, has_side_effects=True, vmem_limit_bytes=60 * 1024 * 1024
        ),
    )(jnp.asarray(table), sections, feed_rate, kill_rate, initial)
    return (result, jnp.max(residual))


def solution(mesh):
    placed = (
        P(None, "space", None),
        P("node", None, "space", None),
        P("space", None),
        P("space", None),
    )
    return jax.shard_map(
        shards,
        mesh=mesh,
        in_specs=placed,
        out_specs=(P("node", None, "space", None), P()),
        check_vma=False,
    )
```

```python
import functools

import jax
import jax.numpy as jnp
import numpy as np
from jax import lax
from jax.experimental import pallas as pl
from jax.experimental.pallas import tpu as pltpu
from jax.sharding import PartitionSpec as P

SWEEPS = 6


step_size = 4.0
diff_u = 1.0
diff_v = 0.5


def radau_target(order, value):
    before = 1.0
    current = value
    previous = 1.0
    for degree in range(1, order):
        following = ((2 * degree + 1) * value * current - degree * before) / (degree + 1)
        before = current
        current = following
    previous = before
    return current - previous


def radau_table(total):
    grid_count = 20000
    roots_found = []
    left_value = -1.0
    left_target = radau_target(total, left_value)
    for step_index in range(1, grid_count):
        right_value = -1.0 + 2.0 * step_index / grid_count
        right_target = radau_target(total, right_value)
        if left_target * right_target < 0.0:
            lower = left_value
            upper = right_value
            lower_target = left_target
            for bisect_index in range(80):
                halfway = 0.5 * (lower + upper)
                halfway_target = radau_target(total, halfway)
                if lower_target * halfway_target <= 0.0:
                    upper = halfway
                else:
                    lower = halfway
                    lower_target = halfway_target
            roots_found.append(0.5 * (lower + upper))
        left_value = right_value
        left_target = right_target
    roots_found.append(1.0)
    points = [(value + 1.0) / 2.0 for value in roots_found]
    quad_rows = []
    for node_index in range(total):
        row_values = []
        for basis_index in range(total):
            coefs = [1.0]
            for other_index in range(total):
                if other_index != basis_index:
                    scale = 1.0 / (points[basis_index] - points[other_index])
                    shifted = [0.0] + coefs
                    widened = coefs + [0.0]
                    coefs = [
                        (shifted[k] - points[other_index] * widened[k]) * scale
                        for k in range(len(shifted))
                    ]
            integral = 0.0
            for power_index in range(len(coefs)):
                integral += (
                    coefs[power_index] * points[node_index] ** (power_index + 1) / (power_index + 1)
                )
            row_values.append(integral)
        quad_rows.append(row_values)
    return (np.array(points), np.array(quad_rows))


MESH = pl.DeviceIdType.MESH
LANES = 128
EDGE = 8
TOP = 2 * EDGE
SLOPE_TILES = 2
MIX_TILES = 2
GATHER_TILES = 4
SWEEP_TILES = 32
SWEEP_ROWS = 8


def grouped(total, most):
    return max(k for k in range(1, most + 1) if total % k == 0)


def kernel(
    nodes,
    spaces,
    table,
    sections,
    feed_rate,
    kill_rate,
    initial,
    out,
    residual,
    sec,
    feed,
    kill,
    init,
    side,
    slope,
    arrived,
    mixed,
    quad,
    work_a,
    work_b,
    final,
    peak,
    peaks_node,
    peaks_space,
    local_sem,
    out_sem,
    halo_sem,
    first_sem,
    second_sem,
    side_sem,
    peak_node_sem,
    peak_space_sem,
):
    cols = sec.shape[1]
    rows = slope.shape[2]
    block = cols // nodes
    me = lax.axis_index("node")
    here = lax.axis_index("space")
    tall = 2 if nodes % 2 == 0 else 1
    wide = nodes // tall
    pieces = ((EDGE, rows - 2 * EDGE), (0, EDGE), (rows - EDGE, EDGE))
    mid, edges = 0, (1, 2)

    def ahead(o):
        return ((me // wide + o // wide) % tall) * wide + (me % wide + o % wide) % wide

    def behind(o):
        return ((me // wide + tall - o // wide) % tall) * wide + (
            me % wide + wide - o % wide
        ) % wide

    def fetch(source, target, sem):
        def one(c, carry):
            at = pl.ds(pl.multiple_of(c * LANES, LANES), LANES)
            pltpu.make_async_copy(source.at[:, at], target(c), sem).start()
            return carry

        lax.fori_loop(0, cols, one, 0)

    own_rows = pl.ds(TOP, rows)
    for s in range(2):
        fetch(sections.at[0, s], lambda c: sec.at[s, c, own_rows], local_sem.at[s])
    fetch(feed_rate, lambda c: feed.at[c], local_sem.at[2])
    fetch(kill_rate, lambda c: kill.at[c], local_sem.at[3])

    barrier = pltpu.get_barrier_semaphore()
    for o in range(1, nodes):
        pl.semaphore_signal(barrier, inc=1, device_id={"node": ahead(o)}, device_id_type=MESH)
    for o in range(1, spaces):
        pl.semaphore_signal(
            barrier, inc=1, device_id={"space": (here + o) % spaces}, device_id_type=MESH
        )

    def arrived_in(ref, sem):
        pltpu.make_async_copy(ref, ref, sem).wait()

    def halo(ref, sem, s, way):
        start = TOP + rows - EDGE if way == 0 else TOP
        land = TOP - EDGE if way == 0 else TOP + rows
        other = (here + 1) % spaces if way == 0 else (here + spaces - 1) % spaces
        return pltpu.make_async_remote_copy(
            src_ref=ref.at[s, :, pl.ds(start, EDGE)],
            dst_ref=ref.at[s, :, pl.ds(land, EDGE)],
            send_sem=sem.at[0, s, way],
            recv_sem=sem.at[1, s, way],
            device_id={"space": other},
            device_id_type=MESH,
        )

    def first(s, p, o):
        start, size = pieces[p]
        return pltpu.make_async_remote_copy(
            src_ref=slope.at[s, pl.ds(ahead(o) * block, block), pl.ds(start, size)],
            dst_ref=arrived.at[o - 1, s, :, pl.ds(start, size)],
            send_sem=first_sem.at[0, s, p, o - 1],
            recv_sem=first_sem.at[1, s, p, o - 1],
            device_id={"node": ahead(o)},
            device_id_type=MESH,
        )

    def second(s, p, o):
        start, size = pieces[p]
        return pltpu.make_async_remote_copy(
            src_ref=mixed.at[o - 1, s, :, pl.ds(start, size)],
            dst_ref=quad.at[s, pl.ds(me * block, block), pl.ds(start, size)],
            send_sem=second_sem.at[0, s, p, o - 1],
            recv_sem=second_sem.at[1, s, p, o - 1],
            device_id={"node": ahead(o)},
            device_id_type=MESH,
        )

    arrived_in(sec.at[0, :, own_rows], local_sem.at[0])
    arrived_in(sec.at[1, :, own_rows], local_sem.at[1])
    pl.semaphore_wait(barrier, nodes - 1 + spaces - 1)
    for s in range(2):
        for way in range(2):
            halo(sec, halo_sem, s, way).start()
    arrived_in(feed, local_sem.at[2])
    arrived_in(kill, local_sem.at[3])
    for s in range(2):
        fetch(initial.at[s], lambda c: init.at[s, c], local_sem.at[4 + s])

    own_step = table[nodes * nodes + me]
    coupling = (own_step * diff_u, own_step * diff_v)

    def around(ref, s, c, count, start, size):
        lane = lax.broadcasted_iota(jnp.int32, (size, LANES), 1)
        at = pl.ds(start, size)
        where = [(c + cols - 1) % cols] + [c + k for k in range(count)] + [(c + count) % cols]
        tiles = [ref[s, k, at, :] for k in where]
        sums = []
        for k in range(1, count + 1):
            left = pltpu.roll(jnp.where(lane == LANES - 1, tiles[k - 1], tiles[k]), 1, 1)
            right = pltpu.roll(jnp.where(lane == 0, tiles[k + 1], tiles[k]), LANES - 1, 1)
            below = ref[s, where[k], pl.ds(start + 1, size), :]
            above = ref[s, where[k], pl.ds(start - 1, size), :]
            sums.append((below + above) + (right + left))
        return tiles[1:-1], sums

    def slopes(owner, p):
        start, size = pieces[p]
        at = pl.ds(start, size)
        group = grouped(block, SLOPE_TILES if size > EDGE else 8)

        def one(g, carry):
            c = owner * block + g * group
            us, u_rings = around(sec, 0, c, group, TOP + start, size)
            vs, v_rings = around(sec, 1, c, group, TOP + start, size)
            for k in range(group):
                u, v = us[k], vs[k]
                f = feed[c + k, at, :]
                u_lap = diff_u * (u_rings[k] - 4.0 * u)
                v_lap = diff_v * (v_rings[k] - 4.0 * v)
                product = u * v * v
                slope[0, c + k, at, :] = u_lap + (f * (1.0 - u) - product)
                slope[1, c + k, at, :] = v_lap + (product - (f + kill[c + k, at, :]) * v)
                side[0, c + k, pl.ds(TOP + start, size), :] = own_step * u_lap
                side[1, c + k, pl.ds(TOP + start, size), :] = own_step * v_lap
            return carry

        lax.fori_loop(0, block // group, one, 0)

    order = tuple(range(nodes - 1, 0, -1))
    for o in order:
        slopes(ahead(o), mid)
        first(0, mid, o).start()
    for s in range(2):
        for way in range(2):
            halo(sec, halo_sem, s, way).wait_recv()
    for o in order:
        for p in edges:
            slopes(ahead(o), p)
            first(0, p, o).start()
    for o in order:
        first(1, mid, o).start()
    for o in order:
        for p in edges:
            first(1, p, o).start()
    for p in range(3):
        slopes(me, p)

    sources = [me] + [behind(o) for o in range(1, nodes)]
    targets = [me] + [ahead(o) for o in range(1, nodes)]
    weights = [[table[m * nodes + j] for j in sources] for m in targets]

    def mix(s, p):
        start, size = pieces[p]
        at = pl.ds(start, size)
        group = grouped(block, MIX_TILES if size > EDGE else 8)

        def one(g, carry):
            for i in range(group):
                k = g * group + i
                values = [slope[s, me * block + k, at, :]] + [
                    arrived[o - 1, s, k, at, :] for o in range(1, nodes)
                ]
                for t, weight in enumerate(weights):
                    total = weight[0] * values[0]
                    for j in range(1, nodes):
                        total = total + weight[j] * values[j]
                    if t == 0:
                        quad[s, me * block + k, at, :] = total
                    else:
                        mixed[t - 1, s, k, at, :] = total
            return carry

        lax.fori_loop(0, block // group, one, 0)

    for s in range(2):
        for o in order:
            for p in edges + (mid,):
                first(s, p, o).wait_recv()
        for p in edges + (mid,):
            mix(s, p)
            for o in order:
                second(s, p, o).start()

    inverse = [1.0 / (4.0 * c + 1.0) for c in coupling]

    def gather(s, p, worst):
        start, size = pieces[p]
        at = pl.ds(start, size)
        for o in order:
            second(s, p, o).wait_recv()

        group = grouped(cols, GATHER_TILES if size > EDGE else 8)
        where = pl.ds(TOP + start, size)

        def one(g, worst):
            for k in range(group):
                c = g * group + k
                whole = init[s, c, at, :] + quad[s, c, at, :]
                gap = jnp.abs(whole - sec[s, c, where, :])
                side[s, c, where, :] = (whole - side[s, c, where, :]) * inverse[s]
                worst = jnp.maximum(worst, jnp.max(gap.reshape(size // EDGE, EDGE, LANES), axis=0))
            return worst

        return lax.fori_loop(0, cols // group, one, worst)

    def sweep(s, source, plane, first_row, size, put):
        factor = coupling[s] * inverse[s]
        group = grouped(cols, SWEEP_TILES)

        for low in range(first_row, first_row + size, SWEEP_ROWS):
            high = min(SWEEP_ROWS, first_row + size - low)

            def one(g, carry):
                c = g * group
                _, sums = around(source, plane, c, group, low, high)
                for k in range(group):
                    put(c + k, low, high, side[s, c + k, pl.ds(low, high), :] + factor * sums[k])
                return carry

            lax.fori_loop(0, cols // group, one, 0)

    def peak_node(o):
        return pltpu.make_async_remote_copy(
            src_ref=peak.at[0],
            dst_ref=peaks_node.at[o - 1],
            send_sem=peak_node_sem.at[0, o - 1],
            recv_sem=peak_node_sem.at[1, o - 1],
            device_id={"node": ahead(o)},
            device_id_type=MESH,
        )

    def peak_space(o):
        return pltpu.make_async_remote_copy(
            src_ref=peak.at[1],
            dst_ref=peaks_space.at[o - 1],
            send_sem=peak_space_sem.at[0, o - 1],
            recv_sem=peak_space_sem.at[1, o - 1],
            device_id={"space": (here + o) % spaces},
            device_id_type=MESH,
        )

    def fold_node():
        for o in range(1, nodes):
            peak_node(o).wait_recv()
        peak[1] = jnp.maximum(peak[0], jnp.max(peaks_node[...], axis=0))
        for o in range(1, spaces):
            peak_space(o).start()

    works = (work_a, work_b)
    worst = jnp.zeros((EDGE, LANES), jnp.float32)
    for s in range(2):
        arrived_in(init.at[s], local_sem.at[4 + s])
        for p in edges:
            worst = gather(s, p, worst)
        for way in range(2):
            halo(side, side_sem, s, way).start()
        worst = gather(s, mid, worst)
        if s == 1:
            peak[0] = worst
            for o in range(1, nodes):
                peak_node(o).start()
        for way in range(2):
            halo(side, side_sem, s, way).wait_recv()

        def into(ref):
            def put(c, low, high, value):
                ref[0, c, pl.ds(low, high), :] = value

            return put

        def put_final(c, low, high, value):
            final[s, c, pl.ds(low - TOP, high), :] = value

        for index in range(SWEEPS):
            source, plane = (sec, s) if index == 0 else (works[(index + 1) % 2], 0)
            if index == SWEEPS - 1:
                if s == 1:
                    fold_node()
                sweep(s, source, plane, TOP, rows, put_final)
            else:
                sweep(s, source, plane, TOP - EDGE, rows + 2 * EDGE, into(works[index % 2]))

        def give(c, carry):
            at = pl.ds(pl.multiple_of(c * LANES, LANES), LANES)
            pltpu.make_async_copy(final.at[s, c], out.at[0, s, :, at], out_sem.at[s]).start()
            return carry

        lax.fori_loop(0, cols, give, 0)

    for o in range(1, spaces):
        peak_space(o).wait_recv()
    residual[0, 0] = jnp.max(jnp.maximum(peak[1], jnp.max(peaks_space[...], axis=0)))
    for s in range(2):
        for way in range(2):
            halo(sec, halo_sem, s, way).wait_send()
            halo(side, side_sem, s, way).wait_send()
        for p in range(3):
            for o in order:
                first(s, p, o).wait_send()
                second(s, p, o).wait_send()
    for o in range(1, nodes):
        peak_node(o).wait_send()
    for o in range(1, spaces):
        peak_space(o).wait_send()
    for s in range(2):
        arrived_in(final.at[s], out_sem.at[s])


def shards(initial, sections, feed_rate, kill_rate):
    nodes = lax.axis_size("node")
    spaces = lax.axis_size("space")
    rows, columns = feed_rate.shape
    cols = columns // LANES
    block = cols // nodes
    points, quad_matrix = radau_table(nodes)
    table = np.concatenate(
        [
            step_size * np.float32(quad_matrix).reshape(-1),
            step_size * np.float32(points),
        ]
    ).astype(np.float32)
    high = TOP + rows + TOP
    f32 = jnp.float32
    any_spec = pl.BlockSpec(memory_space=pl.ANY)
    result, residual = pl.pallas_call(
        functools.partial(kernel, nodes, spaces),
        out_shape=(
            jax.ShapeDtypeStruct(sections.shape, f32),
            jax.ShapeDtypeStruct((1, 1), f32),
        ),
        in_specs=[pl.BlockSpec(memory_space=pltpu.SMEM)] + [any_spec] * 4,
        out_specs=(any_spec, pl.BlockSpec(memory_space=pltpu.SMEM)),
        scratch_shapes=[
            pltpu.VMEM((2, cols, high, LANES), f32),
            pltpu.VMEM((cols, rows, LANES), f32),
            pltpu.VMEM((cols, rows, LANES), f32),
            pltpu.VMEM((2, cols, rows, LANES), f32),
            pltpu.VMEM((2, cols, high, LANES), f32),
            pltpu.VMEM((2, cols, rows, LANES), f32),
            pltpu.VMEM((nodes - 1, 2, block, rows, LANES), f32),
            pltpu.VMEM((nodes - 1, 2, block, rows, LANES), f32),
            pltpu.VMEM((2, cols, rows, LANES), f32),
            pltpu.VMEM((1, cols, high, LANES), f32),
            pltpu.VMEM((1, cols, high, LANES), f32),
            pltpu.VMEM((2, cols, rows, LANES), f32),
            pltpu.VMEM((2, EDGE, LANES), f32),
            pltpu.VMEM((nodes - 1, EDGE, LANES), f32),
            pltpu.VMEM((spaces - 1, EDGE, LANES), f32),
            pltpu.SemaphoreType.DMA((6,)),
            pltpu.SemaphoreType.DMA((2,)),
            pltpu.SemaphoreType.DMA((2, 2, 2)),
            pltpu.SemaphoreType.DMA((2, 2, 3, nodes - 1)),
            pltpu.SemaphoreType.DMA((2, 2, 3, nodes - 1)),
            pltpu.SemaphoreType.DMA((2, 2, 2)),
            pltpu.SemaphoreType.DMA((2, nodes - 1)),
            pltpu.SemaphoreType.DMA((2, spaces - 1)),
        ],
        compiler_params=pltpu.CompilerParams(
            collective_id=0, has_side_effects=True, vmem_limit_bytes=60 * 1024 * 1024
        ),
    )(jnp.asarray(table), sections, feed_rate, kill_rate, initial)
    return (result, residual.reshape(()))


def solution(mesh):
    placed = (
        P(None, "space", None),
        P("node", None, "space", None),
        P("space", None),
        P("space", None),
    )
    return jax.shard_map(
        shards,
        mesh=mesh,
        in_specs=placed,
        out_specs=(P("node", None, "space", None), P()),
        check_vma=False,
    )
```

```python
import functools

import jax
import jax.numpy as jnp
import numpy as np
from jax import lax
from jax.experimental import pallas as pl
from jax.experimental.pallas import tpu as pltpu
from jax.sharding import PartitionSpec as P

SWEEPS = 6


step_size = 4.0
diff_u = 1.0
diff_v = 0.5


def radau_target(order, value):
    before = 1.0
    current = value
    previous = 1.0
    for degree in range(1, order):
        following = ((2 * degree + 1) * value * current - degree * before) / (degree + 1)
        before = current
        current = following
    previous = before
    return current - previous


def radau_table(total):
    grid_count = 20000
    roots_found = []
    left_value = -1.0
    left_target = radau_target(total, left_value)
    for step_index in range(1, grid_count):
        right_value = -1.0 + 2.0 * step_index / grid_count
        right_target = radau_target(total, right_value)
        if left_target * right_target < 0.0:
            lower = left_value
            upper = right_value
            lower_target = left_target
            for bisect_index in range(80):
                halfway = 0.5 * (lower + upper)
                halfway_target = radau_target(total, halfway)
                if lower_target * halfway_target <= 0.0:
                    upper = halfway
                else:
                    lower = halfway
                    lower_target = halfway_target
            roots_found.append(0.5 * (lower + upper))
        left_value = right_value
        left_target = right_target
    roots_found.append(1.0)
    points = [(value + 1.0) / 2.0 for value in roots_found]
    quad_rows = []
    for node_index in range(total):
        row_values = []
        for basis_index in range(total):
            coefs = [1.0]
            for other_index in range(total):
                if other_index != basis_index:
                    scale = 1.0 / (points[basis_index] - points[other_index])
                    shifted = [0.0] + coefs
                    widened = coefs + [0.0]
                    coefs = [
                        (shifted[k] - points[other_index] * widened[k]) * scale
                        for k in range(len(shifted))
                    ]
            integral = 0.0
            for power_index in range(len(coefs)):
                integral += (
                    coefs[power_index] * points[node_index] ** (power_index + 1) / (power_index + 1)
                )
            row_values.append(integral)
        quad_rows.append(row_values)
    return (np.array(points), np.array(quad_rows))


MESH = pl.DeviceIdType.MESH
LANES = 128
EDGE = 8
TOP = 2 * EDGE
SLOPE_TILES = 2
MIX_TILES = 2
GATHER_TILES = 4
LATE = 16


def grouped(total, most):
    return max(k for k in range(1, most + 1) if total % k == 0)


def kernel(
    nodes,
    spaces,
    table,
    sections,
    feed_rate,
    kill_rate,
    initial,
    out,
    residual,
    sec,
    feed,
    kill,
    init,
    side,
    slope,
    arrived,
    mixed,
    quad,
    works_a,
    works_b,
    works_c,
    works_d,
    works_e,
    peak,
    peaks_node,
    peaks_space,
    local_sem,
    halo_sem,
    first_sem,
    second_sem,
    side_sem,
    peak_node_sem,
    peak_space_sem,
):
    works = (works_a, works_b, works_c, works_d, works_e)
    cols = sec.shape[1]
    rows = slope.shape[2]
    block = cols // nodes
    me = lax.axis_index("node")
    here = lax.axis_index("space")
    tall = 2 if nodes % 2 == 0 else 1
    wide = nodes // tall
    early = rows - 2 * EDGE - LATE
    pieces = (
        (EDGE, early),
        (EDGE + early, LATE),
        (0, EDGE),
        (rows - EDGE, EDGE),
    )
    mids, edges = (0, 1), (2, 3)

    def ahead(o):
        return ((me // wide + o // wide) % tall) * wide + (me % wide + o % wide) % wide

    def behind(o):
        return ((me // wide + tall - o // wide) % tall) * wide + (
            me % wide + wide - o % wide
        ) % wide

    def fetch(source, target, offset, sem):
        for k in range(rows // EDGE):
            pltpu.make_async_copy(
                source.at[k], target.at[:, pl.ds(offset + k * EDGE, EDGE)], sem
            ).start()

    own_rows = pl.ds(TOP, rows)
    for s in range(2):
        fetch(sections.at[s], sec.at[s], TOP, local_sem.at[s])
    fetch(feed_rate, feed, 0, local_sem.at[2])
    fetch(kill_rate, kill, 0, local_sem.at[3])

    barrier = pltpu.get_barrier_semaphore()
    for o in range(1, nodes):
        pl.semaphore_signal(barrier, inc=1, device_id={"node": ahead(o)}, device_id_type=MESH)
    for o in range(1, spaces):
        pl.semaphore_signal(
            barrier, inc=1, device_id={"space": (here + o) % spaces}, device_id_type=MESH
        )

    def arrived_in(ref, sem):
        pltpu.make_async_copy(ref, ref, sem).wait()

    def halo(ref, sem, s, way):
        start = TOP + rows - EDGE if way == 0 else TOP
        land = TOP - EDGE if way == 0 else TOP + rows
        other = (here + 1) % spaces if way == 0 else (here + spaces - 1) % spaces
        return pltpu.make_async_remote_copy(
            src_ref=ref.at[s, :, pl.ds(start, EDGE)],
            dst_ref=ref.at[s, :, pl.ds(land, EDGE)],
            send_sem=sem.at[0, s, way],
            recv_sem=sem.at[1, s, way],
            device_id={"space": other},
            device_id_type=MESH,
        )

    def first(s, p, o):
        start, size = pieces[p]
        return pltpu.make_async_remote_copy(
            src_ref=slope.at[s, pl.ds(ahead(o) * block, block), pl.ds(start, size)],
            dst_ref=arrived.at[o - 1, s, :, pl.ds(start, size)],
            send_sem=first_sem.at[0, s, p, o - 1],
            recv_sem=first_sem.at[1, s, p, o - 1],
            device_id={"node": ahead(o)},
            device_id_type=MESH,
        )

    def second(s, p, o):
        start, size = pieces[p]
        return pltpu.make_async_remote_copy(
            src_ref=mixed.at[o - 1, s, :, pl.ds(start, size)],
            dst_ref=quad.at[s, pl.ds(me * block, block), pl.ds(start, size)],
            send_sem=second_sem.at[0, s, p, o - 1],
            recv_sem=second_sem.at[1, s, p, o - 1],
            device_id={"node": ahead(o)},
            device_id_type=MESH,
        )

    arrived_in(sec.at[0, :, own_rows], local_sem.at[0])
    arrived_in(sec.at[1, :, own_rows], local_sem.at[1])
    pl.semaphore_wait(barrier, nodes - 1 + spaces - 1)
    for s in range(2):
        for way in range(2):
            halo(sec, halo_sem, s, way).start()
    arrived_in(feed, local_sem.at[2])
    arrived_in(kill, local_sem.at[3])
    for s in range(2):
        fetch(initial.at[s], init.at[s], 0, local_sem.at[4 + s])

    own_step = table[nodes * nodes + me]
    coupling = (own_step * diff_u, own_step * diff_v)

    def around(ref, s, c, count, start, size):
        lane = lax.broadcasted_iota(jnp.int32, (size, LANES), 1)
        at = pl.ds(start, size)
        where = [(c + cols - 1) % cols] + [c + k for k in range(count)] + [(c + count) % cols]
        tiles = [ref[s, k, at, :] for k in where]
        sums = []
        for k in range(1, count + 1):
            left = pltpu.roll(jnp.where(lane == LANES - 1, tiles[k - 1], tiles[k]), 1, 1)
            right = pltpu.roll(jnp.where(lane == 0, tiles[k + 1], tiles[k]), LANES - 1, 1)
            below = ref[s, where[k], pl.ds(start + 1, size), :]
            above = ref[s, where[k], pl.ds(start - 1, size), :]
            sums.append((below + above) + (right + left))
        return tiles[1:-1], sums

    def slopes(owner, p):
        start, size = pieces[p]
        at = pl.ds(start, size)
        group = grouped(block, SLOPE_TILES if size > EDGE else 8)

        def one(g, carry):
            c = owner * block + g * group
            us, u_rings = around(sec, 0, c, group, TOP + start, size)
            vs, v_rings = around(sec, 1, c, group, TOP + start, size)
            for k in range(group):
                u, v = us[k], vs[k]
                f = feed[c + k, at, :]
                u_lap = diff_u * (u_rings[k] - 4.0 * u)
                v_lap = diff_v * (v_rings[k] - 4.0 * v)
                product = u * v * v
                slope[0, c + k, at, :] = u_lap + (f * (1.0 - u) - product)
                slope[1, c + k, at, :] = v_lap + (product - (f + kill[c + k, at, :]) * v)
                side[0, c + k, pl.ds(TOP + start, size), :] = own_step * u_lap
                side[1, c + k, pl.ds(TOP + start, size), :] = own_step * v_lap
            return carry

        lax.fori_loop(0, block // group, one, 0)

    order = tuple(range(nodes - 1, 0, -1))
    for o in order:
        for p in mids:
            slopes(ahead(o), p)
            first(0, p, o).start()
    for s in range(2):
        for way in range(2):
            halo(sec, halo_sem, s, way).wait_recv()
    for o in order:
        for p in edges:
            slopes(ahead(o), p)
            first(0, p, o).start()
    for o in order:
        for p in mids:
            first(1, p, o).start()
    for o in order:
        for p in edges:
            first(1, p, o).start()
    for p in mids + edges:
        slopes(me, p)

    sources = [me] + [behind(o) for o in range(1, nodes)]
    targets = [me] + [ahead(o) for o in range(1, nodes)]
    weights = [[table[m * nodes + j] for j in sources] for m in targets]

    def mix(s, p):
        start, size = pieces[p]
        at = pl.ds(start, size)
        group = grouped(block, MIX_TILES if size > EDGE else 8)

        def one(g, carry):
            for i in range(group):
                k = g * group + i
                values = [slope[s, me * block + k, at, :]] + [
                    arrived[o - 1, s, k, at, :] for o in range(1, nodes)
                ]
                for t, weight in enumerate(weights):
                    total = weight[0] * values[0]
                    for j in range(1, nodes):
                        total = total + weight[j] * values[j]
                    if t == 0:
                        quad[s, me * block + k, at, :] = total
                    else:
                        mixed[t - 1, s, k, at, :] = total
            return carry

        lax.fori_loop(0, block // group, one, 0)

    for s in range(2):
        for o in order:
            for p in edges + mids:
                first(s, p, o).wait_recv()
        for p in edges + mids:
            mix(s, p)
            for o in order:
                second(s, p, o).start()

    inverse = [1.0 / (4.0 * c + 1.0) for c in coupling]

    def gather(s, p, worst):
        start, size = pieces[p]
        at = pl.ds(start, size)
        for o in order:
            second(s, p, o).wait_recv()

        group = grouped(cols, GATHER_TILES if size > EDGE else 8)
        where = pl.ds(TOP + start, size)

        def one(g, worst):
            for k in range(group):
                c = g * group + k
                whole = init[s, c, at, :] + quad[s, c, at, :]
                gap = jnp.abs(whole - sec[s, c, where, :])
                side[s, c, where, :] = (whole - side[s, c, where, :]) * inverse[s]
                worst = jnp.maximum(worst, jnp.max(gap.reshape(size // EDGE, EDGE, LANES), axis=0))
            return worst

        return lax.fori_loop(0, cols // group, one, worst)

    bottom = TOP + rows + SWEEPS - 1
    split = bottom - 2 * LATE

    def band(s, i):
        factor = coupling[s] * inverse[s]
        for k in range(SWEEPS):
            start = TOP - SWEEPS + 1 + k if i == 0 else split - k
            stop = split - k if i == 0 else bottom - k
            source, plane = (sec, s) if k == 0 else (works[k - 1], 0)
            for low in range(start, stop, EDGE):
                size = min(EDGE, stop - low)
                _, sums = around(source, plane, 0, cols, low, size)
                for c in range(cols):
                    value = side[s, c, pl.ds(low, size), :] + factor * sums[c]
                    if k == SWEEPS - 1:
                        out[s, (low - TOP) // EDGE, c] = value
                    else:
                        works[k][0, c, pl.ds(low, size), :] = value

    def peak_node(o):
        return pltpu.make_async_remote_copy(
            src_ref=peak.at[0],
            dst_ref=peaks_node.at[o - 1],
            send_sem=peak_node_sem.at[0, o - 1],
            recv_sem=peak_node_sem.at[1, o - 1],
            device_id={"node": ahead(o)},
            device_id_type=MESH,
        )

    def peak_space(o):
        return pltpu.make_async_remote_copy(
            src_ref=peak.at[1],
            dst_ref=peaks_space.at[o - 1],
            send_sem=peak_space_sem.at[0, o - 1],
            recv_sem=peak_space_sem.at[1, o - 1],
            device_id={"space": (here + o) % spaces},
            device_id_type=MESH,
        )

    def fold_node():
        for o in range(1, nodes):
            peak_node(o).wait_recv()
        peak[1] = jnp.maximum(peak[0], jnp.max(peaks_node[...], axis=0))
        for o in range(1, spaces):
            peak_space(o).start()

    worst = jnp.zeros((EDGE, LANES), jnp.float32)
    for s in range(2):
        arrived_in(init.at[s], local_sem.at[4 + s])
        for p in edges:
            worst = gather(s, p, worst)
        for way in range(2):
            halo(side, side_sem, s, way).start()
        worst = gather(s, mids[0], worst)
        for way in range(2):
            halo(side, side_sem, s, way).wait_recv()
        band(s, 0)
        worst = gather(s, mids[1], worst)
        if s == 1:
            peak[0] = worst
            for o in range(1, nodes):
                peak_node(o).start()
        band(s, 1)
        if s == 1:
            fold_node()

    for o in range(1, spaces):
        peak_space(o).wait_recv()
    residual[0, 0] = jnp.max(jnp.maximum(peak[1], jnp.max(peaks_space[...], axis=0)))
    for s in range(2):
        for way in range(2):
            halo(sec, halo_sem, s, way).wait_send()
            halo(side, side_sem, s, way).wait_send()
        for p in mids + edges:
            for o in order:
                first(s, p, o).wait_send()
                second(s, p, o).wait_send()
    for o in range(1, nodes):
        peak_node(o).wait_send()
    for o in range(1, spaces):
        peak_space(o).wait_send()


def shards(initial, sections, feed_rate, kill_rate):
    nodes = lax.axis_size("node")
    spaces = lax.axis_size("space")
    rows, columns = feed_rate.shape
    cols = columns // LANES
    block = cols // nodes
    points, quad_matrix = radau_table(nodes)
    table = np.concatenate(
        [
            step_size * np.float32(quad_matrix).reshape(-1),
            step_size * np.float32(points),
        ]
    ).astype(np.float32)
    high = TOP + rows + TOP
    f32 = jnp.float32

    def tiled(array):
        split = array.reshape(*array.shape[:-2], rows // EDGE, EDGE, cols, LANES)
        return jnp.swapaxes(split, -3, -2)

    any_spec = pl.BlockSpec(memory_space=pl.ANY)
    result, residual = pl.pallas_call(
        functools.partial(kernel, nodes, spaces),
        out_shape=(
            pltpu.VMEM((2, rows // EDGE, cols, EDGE, LANES), f32),
            jax.ShapeDtypeStruct((1, 1), f32),
        ),
        in_specs=[pl.BlockSpec(memory_space=pltpu.SMEM)] + [any_spec] * 4,
        out_specs=(pl.BlockSpec(memory_space=pltpu.VMEM), pl.BlockSpec(memory_space=pltpu.SMEM)),
        scratch_shapes=[
            pltpu.VMEM((2, cols, high, LANES), f32),
            pltpu.VMEM((cols, rows, LANES), f32),
            pltpu.VMEM((cols, rows, LANES), f32),
            pltpu.VMEM((2, cols, rows, LANES), f32),
            pltpu.VMEM((2, cols, high, LANES), f32),
            pltpu.VMEM((2, cols, rows, LANES), f32),
            pltpu.VMEM((nodes - 1, 2, block, rows, LANES), f32),
            pltpu.VMEM((nodes - 1, 2, block, rows, LANES), f32),
            pltpu.VMEM((2, cols, rows, LANES), f32),
            *[pltpu.VMEM((1, cols, high, LANES), f32)] * (SWEEPS - 1),
            pltpu.VMEM((2, EDGE, LANES), f32),
            pltpu.VMEM((nodes - 1, EDGE, LANES), f32),
            pltpu.VMEM((spaces - 1, EDGE, LANES), f32),
            pltpu.SemaphoreType.DMA((6,)),
            pltpu.SemaphoreType.DMA((2, 2, 2)),
            pltpu.SemaphoreType.DMA((2, 2, 4, nodes - 1)),
            pltpu.SemaphoreType.DMA((2, 2, 4, nodes - 1)),
            pltpu.SemaphoreType.DMA((2, 2, 2)),
            pltpu.SemaphoreType.DMA((2, nodes - 1)),
            pltpu.SemaphoreType.DMA((2, spaces - 1)),
        ],
        compiler_params=pltpu.CompilerParams(
            collective_id=0, has_side_effects=True, vmem_limit_bytes=61 * 1024 * 1024
        ),
    )(jnp.asarray(table), *[tiled(a) for a in (sections[0], feed_rate, kill_rate, initial)])
    result = jnp.swapaxes(result, -3, -2).reshape(sections.shape)
    return (result, residual.reshape(()))


def solution(mesh):
    placed = (
        P(None, "space", None),
        P("node", None, "space", None),
        P("space", None),
        P("space", None),
    )
    return jax.shard_map(
        shards,
        mesh=mesh,
        in_specs=placed,
        out_specs=(P("node", None, "space", None), P()),
        check_vma=False,
    )
```
